32 devices in a mesh: blk: 8 (over y, x, core), walk: 4 (over z).
Axes of the slice: x: 2, y: 2, z: 4, core: 2. Of those that a mesh axis runs over, the one named last changes fastest.
Arguments:
- walker_m: bfloat16 [4, 8, 128, 128], P('walk', 'blk'), may hold values from -6 to 6
- vertex_times: int32 [4, 8, 128], P('walk', 'blk'), may hold values from 0 to 1023
- vertex_labels: int32 [4, 8, 128], P('walk', 'blk'), may hold values from 0 to 35
- freq_index: int32 [24], replicated, may hold values from -64 to 63
- q_index: int32 [8], P('blk'), may hold values from 0 to 35
Outputs:
- g4: float32 [8, 2, 864, 864], P('blk', None, 'walk')
The draws below stay inside these ranges and needn't reach their ends.
Inputs may be any that keep to these rules, and one draw needn't show every extreme that they name: `q_index`: entry b is 6 qx + qy for the transfer momentum (qx, qy). `freq_index`: frequency f is pi (2 n + 1) / beta with n its entry. `vertex_times`: the time is entry * beta / 1024. `vertex_labels`: site s lies at row s // 6 and column s mod 6 of the 6×6 cluster.
All inputs are finite; a program needn't handle non-finite values.
Results may differ from the reference program's by a relative error of at most 0.0061.
Values may be sent and summed in bfloat16 or wider, within the bound.
A program may use at most 128 MiB of HBM per device.

```python
import math
import jax
import jax.numpy as jnp
from jax import lax

SIDE = 6
NK = 36
NF = 24
K = 864
V = 128
STEPS = 4
TGRID = 1024
OWNERS = 8
GROUPS = 4
N_BLK = 8
N_WALK = 4


def touch_ends(drawn, key, low, high):
    dims = drawn.shape
    place = [jax.random.randint(jax.random.fold_in(key, axis), (), 0, dims[axis]) for axis in range(len(dims))]
    drawn = drawn.at[tuple(place)].set(low)
    longest = dims.index(max(dims))
    place[longest] = (place[longest] + 1) % dims[longest]
    return drawn.at[tuple(place)].set(high)


def block_levels(stream_key, dims, cuts, least, top_value):
    def one(dim, blocks):
        draws = jax.random.uniform(jax.random.fold_in(jax.random.fold_in(stream_key, 6), dim), (blocks,), jnp.float32, least / len(cuts), top_value / len(cuts))
        return jnp.repeat(jnp.exp(draws), dims[dim] // blocks).reshape((-1,) + (1,) * (len(dims) - dim - 1))

    factor_of = one(*cuts[0])
    for cut in cuts[1:]:
        factor_of = factor_of * one(*cut)
    return factor_of


def gaussian(stream_key, dims, width, reach, cuts=(), kind=jnp.bfloat16):
    loudness = block_levels(stream_key, dims, cuts, -0.22, 0.18) if cuts else 1.0
    values = jax.random.normal(stream_key, dims, jnp.float32) * width * loudness
    return jnp.minimum(jnp.maximum(values, -reach), reach).astype(kind)


def setup_inputs(seed: int = 0) -> dict:
    streams_of = jax.random.split(jax.random.key(seed), 6)
    return {
        "walker_m": gaussian(streams_of[0], (GROUPS, OWNERS, V, V), 1.0, 6.0, ((0, 4), (1, 8))),
        "vertex_times": touch_ends(jax.random.randint(streams_of[1], (GROUPS, OWNERS, V), 0, TGRID), jax.random.fold_in(streams_of[1], 1), 0, TGRID - 1).astype(jnp.int32),
        "vertex_labels": touch_ends(jax.random.randint(streams_of[2], (GROUPS, OWNERS, V), 0, NK), jax.random.fold_in(streams_of[2], 1), 0, NK - 1).astype(jnp.int32),
        "freq_index": touch_ends(jax.random.randint(streams_of[3], (NF,), -64, 64), jax.random.fold_in(streams_of[3], 1), -64, 63).astype(jnp.int32),
        "q_index": touch_ends(jax.random.randint(streams_of[4], (OWNERS,), 0, NK), jax.random.fold_in(streams_of[4], 1), 0, NK - 1).astype(jnp.int32),
    }


TWO_PI = 2.0 * math.pi


def phase_tables(time_points, labels, frequencies):
    modulus = 12 * TGRID
    momenta = jnp.arange(NK, dtype=jnp.int32)
    momentum_across = momenta // SIDE
    momentum_down = momenta % SIDE
    site_across = labels // SIDE
    site_down = labels % SIDE
    freq_part = jnp.mod((2 * frequencies[:, None] + 1) * time_points[None, :] * 6, modulus)
    momentum_part = jnp.mod(2 * TGRID * (momentum_across[:, None] * site_across[None, :] + momentum_down[:, None] * site_down[None, :]), modulus)
    phase = jnp.mod(freq_part[None, :, :] - momentum_part[:, None, :], modulus).reshape(NK * NF, -1)
    angles = phase.astype(jnp.float32) * (TWO_PI / modulus)
    return jnp.cos(angles).astype(jnp.bfloat16), jnp.sin(angles).astype(jnp.bfloat16)


def build_green(matrix, time_points, labels, frequencies):
    cos_table, sin_table = phase_tables(time_points, labels, frequencies)
    stacked = jnp.concatenate([cos_table, sin_table], axis=0)
    amplitude = jnp.dot(stacked, matrix, preferred_element_type=jnp.float32).astype(jnp.bfloat16)
    real_part = amplitude[:K]
    imag_part = amplitude[K:]
    left_side = jnp.concatenate([jnp.concatenate([real_part, imag_part], axis=1), jnp.concatenate([imag_part, -real_part], axis=1)], axis=0)
    right_side = jnp.concatenate([cos_table, sin_table], axis=1)
    green_table = lax.dot_general(left_side, right_side, (((1,), (1,)), ((), ())), preferred_element_type=jnp.float32)
    return (green_table * (1.0 / V)).reshape(2, K, K)


def shifted_rows(transfer):
    transfer = transfer.astype(jnp.int32)
    row_index = jnp.arange(K, dtype=jnp.int32)
    momentum = row_index // NF
    offset = row_index % NF
    shift_across = (momentum // SIDE + transfer // SIDE) % SIDE
    shift_down = (momentum % SIDE + transfer % SIDE) % SIDE
    return ((shift_across * SIDE + shift_down) * NF + offset).astype(jnp.int32)


def contribution(green_table, shifted):
    shifted_green = jnp.take(jnp.take(green_table, shifted, axis=1), shifted, axis=2)
    flipped = jnp.swapaxes(green_table, 1, 2)
    real_term = shifted_green[0] * flipped[0] - shifted_green[1] * flipped[1]
    imag_term = shifted_green[0] * flipped[1] + shifted_green[1] * flipped[0]
    return jnp.stack([real_term, imag_term])


def reference(walker_m, vertex_times, vertex_labels, freq_index, q_index):
    walker_count = N_WALK * N_BLK
    matrices = walker_m.reshape(walker_count, V, V)
    time_rows = vertex_times.reshape(walker_count, V)
    label_rows = vertex_labels.reshape(walker_count, V)
    sources = jnp.arange(walker_count, dtype=jnp.int32) % N_BLK

    def visit_walker(running, walker_item):
        matrix, time_points, labels, source = walker_item
        green_table = build_green(matrix, time_points, labels, freq_index)
        for number in range(STEPS):
            offset = number - (STEPS // 2 - 1)
            owner_index = jnp.mod(source - offset, N_BLK).astype(jnp.int32)
            addition = contribution(green_table, shifted_rows(q_index[owner_index]))
            running = running.at[owner_index].add(addition)
        return running, None

    start = jnp.zeros((N_BLK, 2, K, K), jnp.float32)
    running, unused = lax.scan(visit_walker, start, (matrices, time_rows, label_rows, sources))
    return running * (1.0 / (STEPS * N_WALK))
```

```python
import functools
import math

import jax
import jax.numpy as jnp
from jax import lax
from jax.experimental import pallas as pl
from jax.experimental.pallas import tpu as pltpu
from jax.sharding import PartitionSpec as P

SIDE = 6
TGRID = 1024
OFFSETS = (0, 1, -1, 2)


def sine(units):
    wrapped = ((units + 1024) & 2047) - 1024
    folded = jnp.where(wrapped > 512, 1024 - wrapped, wrapped)
    folded = jnp.where(wrapped < -512, -1024 - wrapped, folded)
    x = folded.astype(jnp.float32) * (math.pi / 1024.0)
    y = x * x
    total = jnp.full_like(y, 1.0 / math.factorial(13))
    for order in (11, 9, 7, 5, 3, 1):
        sign = -1.0 if (order // 2) % 2 else 1.0
        total = total * y + sign / math.factorial(order)
    return total * x


def sixth_turn(m):
    r = m - 6 * ((m * 10923) >> 16)
    half = jnp.where((r == 1) | (r == 5), 0.5, -0.5)
    cosine = jnp.where(r == 0, 1.0, jnp.where(r == 3, -1.0, half))
    root = math.sqrt(3.0) / 2.0
    side = jnp.where(r < 3, root, -root)
    return cosine.astype(jnp.float32), jnp.where((r == 0) | (r == 3), 0.0, side).astype(jnp.float32)


def kernel(
    walkers, m_ref, tl_ref, freq_ref, q_ref, out_ref,
    odd, turn_c, turn_s, both, table, moved, left_a, left_b, left_c, right_b,
):
    nf = freq_ref.shape[0]
    v = m_ref.shape[-1]
    nk = SIDE * SIDE
    own_k = out_ref.shape[2] // nf
    cols = out_ref.shape[3]
    first_k = lax.axis_index("walk") * own_k

    row = lax.broadcasted_iota(jnp.int32, (nf, v), 0)
    freq = jnp.zeros((nf, v), jnp.int32)
    for f in range(nf):
        freq = jnp.where(row == f, 2 * freq_ref[f] + 1, freq)
    odd[...] = freq
    both[...] = jnp.zeros_like(both)
    out_ref[...] = jnp.zeros_like(out_ref)
    q = q_ref[0]
    qx = (q * 43) >> 8
    qy = q - SIDE * qx

    def step(i, carry):
        matrix = m_ref[i]
        both[0:v, 0:v] = matrix
        both[v : 2 * v, v : 2 * v] = matrix
        times = tl_ref[i, 0:1]
        labels = tl_ref[i, 1:2]
        sx = (labels * 43) >> 8
        sy = labels - SIDE * sx
        k = lax.broadcasted_iota(jnp.int32, turn_c.shape, 0)
        kx = (k * 43) >> 8
        ky = k - SIDE * kx
        cosines, sines = sixth_turn(kx * sx + ky * sy)
        turn_c[...] = cosines
        turn_s[...] = sines
        cq, sq = sixth_turn(qx * sx + qy * sy)

        units = (odd[...] * times) & 2047
        ca = sine(units + 512)
        sa = sine(units)
        ca_q = ca * cq + sa * sq
        sa_q = sa * cq - ca * sq

        def turned(c, s, k):
            cb = turn_c[pl.ds(k, 1)]
            sb = turn_s[pl.ds(k, 1)]
            return c * cb + s * sb, s * cb - c * sb

        def put(ref, place, first, second, lanes):
            rows = slice(2 * nf * place, 2 * nf * (place + 1))
            ref[rows, lanes] = jnp.concatenate([first, second], axis=0).astype(jnp.bfloat16)

        low, high = slice(0, v), slice(v, 2 * v)
        for pair in range(nk // 2):
            c0, s0 = turned(ca, sa, 2 * pair)
            c1, s1 = turned(ca, sa, 2 * pair + 1)
            put(table, pair, c0, c1, low)
            put(table, pair, s0, s1, high)
            c0, s0 = turned(ca_q, sa_q, 2 * pair)
            c1, s1 = turned(ca_q, sa_q, 2 * pair + 1)
            put(moved, pair, c0, c1, low)
            put(moved, pair, s0, s1, high)
        for j in range(own_k):
            c, s = turned(ca, sa, first_k + j)
            put(left_b, j, c, -s, low)
            put(left_b, j, s, c, high)
            c, s = turned(ca_q, sa_q, first_k + j)
            put(left_c, j, c, s, low)
            put(left_c, j, s, -c, high)

        right_b[...] = jnp.dot(
            table[...], both[...], preferred_element_type=jnp.float32
        ).astype(jnp.bfloat16)
        left_a[...] = jnp.dot(
            left_c[...], both[...], preferred_element_type=jnp.float32
        ).astype(jnp.bfloat16)

        contract = (((1,), (1,)), ((), ()))
        for start in range(0, cols, 256):
            stop = min(start + 256, cols)
            shifted = lax.dot_general(
                left_a[...], moved[start:stop], contract, preferred_element_type=jnp.float32
            )
            flipped = lax.dot_general(
                left_b[...], right_b[start:stop], contract, preferred_element_type=jnp.float32
            )
            for j in range(own_k):
                re = slice(2 * nf * j, 2 * nf * j + nf)
                im = slice(2 * nf * j + nf, 2 * nf * (j + 1))
                rows = slice(nf * j, nf * (j + 1))
                out_ref[0, 0, rows, start:stop] += (
                    shifted[re] * flipped[re] - shifted[im] * flipped[im]
                )
                out_ref[0, 1, rows, start:stop] += (
                    shifted[re] * flipped[im] + shifted[im] * flipped[re]
                )
        return carry

    lax.fori_loop(0, walkers, step, 0)
    scale = 1.0 / (v * v * walkers)
    out_ref[...] = out_ref[...] * scale


def local(walker_m, vertex_times, vertex_labels, freq_index, q_index):
    groups = lax.axis_size("walk")
    owners = lax.axis_size("blk")
    v = walker_m.shape[-1]
    nf = freq_index.shape[0]
    k = SIDE * SIDE * nf
    own = k // groups
    tl = jnp.concatenate([vertex_times[0], vertex_labels[0]], axis=0)
    m = lax.all_gather(walker_m[0, 0], "walk")
    tl = lax.all_gather(tl, "walk")
    ms, tls = [], []
    for d in OFFSETS:
        if d == 0:
            ms.append(m)
            tls.append(tl)
        else:
            pairs = [((b + d) % owners, b) for b in range(owners)]
            ms.append(lax.ppermute(m, "blk", pairs))
            tls.append(lax.ppermute(tl, "blk", pairs))
    m = jnp.concatenate(ms, axis=0)
    tl = jnp.concatenate(tls, axis=0)
    walkers = m.shape[0]
    vmem = pl.BlockSpec(memory_space=pltpu.VMEM)
    smem = pl.BlockSpec(memory_space=pltpu.SMEM)
    bf16 = jnp.bfloat16
    return pl.pallas_call(
        functools.partial(kernel, walkers),
        out_shape=jax.ShapeDtypeStruct((1, 2, own, k), jnp.float32),
        in_specs=[vmem, vmem, smem, smem],
        out_specs=vmem,
        scratch_shapes=[
            pltpu.VMEM((nf, v), jnp.int32),
            pltpu.VMEM((40, v), jnp.float32),
            pltpu.VMEM((40, v), jnp.float32),
            pltpu.VMEM((2 * v, 2 * v), bf16),
            pltpu.VMEM((k, 2 * v), bf16),
            pltpu.VMEM((k, 2 * v), bf16),
            pltpu.VMEM((2 * own, 2 * v), bf16),
            pltpu.VMEM((2 * own, 2 * v), bf16),
            pltpu.VMEM((2 * own, 2 * v), bf16),
            pltpu.VMEM((k, 2 * v), bf16),
        ],
    )(m, tl, freq_index, q_index)


def solution(mesh):
    return jax.shard_map(
        local,
        mesh=mesh,
        in_specs=(
            P("walk", "blk", None, None),
            P("walk", "blk", None),
            P("walk", "blk", None),
            P(),
            P("blk"),
        ),
        out_specs=P("blk", None, "walk", None),
        check_vma=False,
    )
```

```python
import functools
import math

import jax
import jax.numpy as jnp
from jax import lax
from jax.experimental import pallas as pl
from jax.experimental.pallas import tpu as pltpu
from jax.sharding import PartitionSpec as P

SIDE = 6
TGRID = 1024
OFFSETS = (0, 1, -1, 2)
FORWARD = (2, 2, 3)


def sine(units):
    wrapped = ((units + 1024) & 2047) - 1024
    folded = jnp.where(wrapped > 512, 1024 - wrapped, wrapped)
    folded = jnp.where(wrapped < -512, -1024 - wrapped, folded)
    x = folded.astype(jnp.float32) * (math.pi / 1024.0)
    y = x * x
    total = jnp.full_like(y, 1.0 / math.factorial(13))
    for order in (11, 9, 7, 5, 3, 1):
        sign = -1.0 if (order // 2) % 2 else 1.0
        total = total * y + sign / math.factorial(order)
    return total * x


def sixth_turn(m):
    r = m - 6 * ((m * 10923) >> 16)
    half = jnp.where((r == 1) | (r == 5), 0.5, -0.5)
    cosine = jnp.where(r == 0, 1.0, jnp.where(r == 3, -1.0, half))
    root = math.sqrt(3.0) / 2.0
    side = jnp.where(r < 3, root, -root)
    return cosine.astype(jnp.float32), jnp.where((r == 0) | (r == 3), 0.0, side).astype(jnp.float32)


def visits(groups):
    around = sorted(range(1, groups), key=lambda z: min(z, groups - z))
    near = [(0, d) for d in range(len(OFFSETS))]
    far = [(z, 0) for z in around]
    return near + far + [(z, d) for z in around for d in range(1, len(OFFSETS))]


def kernel(
    groups, owners, m_in, t_in, l_in, freq_ref, q_ref, out_ref,
    m_ref, t_ref, l_ref, send_sem, recv_sem,
    odd, turn_c, turn_s, both, table, moved, left_a, left_b, left_c, right_b,
):
    order = visits(groups)
    walkers = len(order)
    w = lax.axis_index("walk")
    b = lax.axis_index("blk")

    def to_walk(z):
        return {"walk": lax.rem(w + groups - z, groups)}

    def to_blk(d):
        return {"blk": lax.rem(b + owners - OFFSETS[d], owners)}

    def copies(sources, slot, device):
        return [
            pltpu.make_async_remote_copy(
                src_ref=source,
                dst_ref=held.at[slot],
                send_sem=send_sem.at[kind, slot],
                recv_sem=recv_sem.at[kind, slot],
                device_id=device,
                device_id_type=pl.DeviceIdType.MESH,
            )
            for kind, (source, held) in enumerate(zip(sources, (m_ref, t_ref, l_ref)))
        ]

    own = (m_in.at[0, 0], t_in.at[0], l_in.at[0])

    def held_at(slot):
        return (m_ref.at[slot], t_ref.at[slot], l_ref.at[slot])

    def arrived(slot):
        for copy in copies(held_at(slot), slot, to_walk(1)):
            copy.wait_recv()

    barrier = pltpu.get_barrier_semaphore()
    peers = [{"walk": lax.rem(w + z, groups)} for z in range(1, groups)]
    reach = sorted({d % owners for d in OFFSETS + tuple(-d for d in OFFSETS)} - {0})
    peers += [{"blk": lax.rem(b + d, owners)} for d in reach]
    for peer in peers:
        pl.semaphore_signal(barrier, inc=1, device_id=peer, device_id_type=pl.DeviceIdType.MESH)
    pl.semaphore_wait(barrier, len(peers))
    for z, d in [o for o in order if o[0] and not o[1]] + [o for o in order if o[1] and not o[0]]:
        for copy in copies(own, order.index((z, d)), to_walk(z) if z else to_blk(d)):
            copy.start()

    def forward(z):
        slot = order.index((z, 0))
        arrived(slot)
        for d in range(1, len(OFFSETS)):
            for copy in copies(held_at(slot), order.index((z, d)), to_blk(d)):
                copy.start()

    m_ref[0] = m_in[0, 0]
    t_ref[0] = t_in[0]
    l_ref[0] = l_in[0]

    nf = freq_ref.shape[0]
    v = m_ref.shape[-1]
    nk = SIDE * SIDE
    own_k = out_ref.shape[2] // nf
    cols = out_ref.shape[3]
    first_k = w * own_k

    row = lax.broadcasted_iota(jnp.int32, (nf, v), 0)
    freq = jnp.zeros((nf, v), jnp.int32)
    for f in range(nf):
        freq = jnp.where(row == f, 2 * freq_ref[f] + 1, freq)
    odd[...] = freq
    both[...] = jnp.zeros_like(both)
    out_ref[...] = jnp.zeros_like(out_ref)
    q = q_ref[0]
    qx = (q * 43) >> 8
    qy = q - SIDE * qx

    def step(i, carry):
        for turn, z in enumerate([z for z, d in order if z and not d]):
            @pl.when(i == FORWARD[min(turn, len(FORWARD) - 1)])
            def _(z=z):
                forward(z)

        first_far = order.index((0, len(OFFSETS) - 1)) + 1
        last_far = first_far + groups - 1

        @pl.when(((i > 0) & (i < first_far)) | (i >= last_far))
        def _():
            arrived(i)

        matrix = m_ref[i]
        both[0:v, 0:v] = matrix
        both[v : 2 * v, v : 2 * v] = matrix
        times = t_ref[i]
        labels = l_ref[i]
        sx = (labels * 43) >> 8
        sy = labels - SIDE * sx
        k = lax.broadcasted_iota(jnp.int32, turn_c.shape, 0)
        kx = (k * 43) >> 8
        ky = k - SIDE * kx
        cosines, sines = sixth_turn(kx * sx + ky * sy)
        turn_c[...] = cosines
        turn_s[...] = sines
        cq, sq = sixth_turn(qx * sx + qy * sy)

        units = (odd[...] * times) & 2047
        ca = sine(units + 512)
        sa = sine(units)
        ca_q = ca * cq + sa * sq
        sa_q = sa * cq - ca * sq

        def turned(c, s, k):
            cb = turn_c[pl.ds(k, 1)]
            sb = turn_s[pl.ds(k, 1)]
            return c * cb + s * sb, s * cb - c * sb

        def put(ref, place, first, second, lanes):
            rows = slice(2 * nf * place, 2 * nf * (place + 1))
            ref[rows, lanes] = jnp.concatenate([first, second], axis=0).astype(jnp.bfloat16)

        low, high = slice(0, v), slice(v, 2 * v)
        for pair in range(nk // 2):
            c0, s0 = turned(ca, sa, 2 * pair)
            c1, s1 = turned(ca, sa, 2 * pair + 1)
            put(table, pair, c0, c1, low)
            put(table, pair, s0, s1, high)
            c0, s0 = turned(ca_q, sa_q, 2 * pair)
            c1, s1 = turned(ca_q, sa_q, 2 * pair + 1)
            put(moved, pair, c0, c1, low)
            put(moved, pair, s0, s1, high)
        for j in range(own_k):
            c, s = turned(ca, sa, first_k + j)
            put(left_b, j, c, -s, low)
            put(left_b, j, s, c, high)
            c, s = turned(ca_q, sa_q, first_k + j)
            put(left_c, j, c, s, low)
            put(left_c, j, s, -c, high)

        right_b[...] = jnp.dot(
            table[...], both[...], preferred_element_type=jnp.float32
        ).astype(jnp.bfloat16)
        left_a[...] = jnp.dot(
            left_c[...], both[...], preferred_element_type=jnp.float32
        ).astype(jnp.bfloat16)

        contract = (((1,), (1,)), ((), ()))
        for start in range(0, cols, 256):
            stop = min(start + 256, cols)
            shifted = lax.dot_general(
                left_a[...], moved[start:stop], contract, preferred_element_type=jnp.float32
            )
            flipped = lax.dot_general(
                left_b[...], right_b[start:stop], contract, preferred_element_type=jnp.float32
            )
            for j in range(own_k):
                re = slice(2 * nf * j, 2 * nf * j + nf)
                im = slice(2 * nf * j + nf, 2 * nf * (j + 1))
                rows = slice(nf * j, nf * (j + 1))
                out_ref[0, 0, rows, start:stop] += (
                    shifted[re] * flipped[re] - shifted[im] * flipped[im]
                )
                out_ref[0, 1, rows, start:stop] += (
                    shifted[re] * flipped[im] + shifted[im] * flipped[re]
                )
        return carry

    lax.fori_loop(0, walkers, step, 0)
    scale = 1.0 / (v * v * walkers)
    out_ref[...] = out_ref[...] * scale
    for slot in range(1, walkers):
        for copy in copies(held_at(slot), slot, to_walk(1)):
            copy.wait_send()


def local(walker_m, vertex_times, vertex_labels, freq_index, q_index):
    groups = lax.axis_size("walk")
    owners = lax.axis_size("blk")
    v = walker_m.shape[-1]
    nf = freq_index.shape[0]
    k = SIDE * SIDE * nf
    own = k // groups
    walkers = groups * len(OFFSETS)
    vmem = pl.BlockSpec(memory_space=pltpu.VMEM)
    smem = pl.BlockSpec(memory_space=pltpu.SMEM)
    bf16 = jnp.bfloat16
    return pl.pallas_call(
        functools.partial(kernel, groups, owners),
        out_shape=jax.ShapeDtypeStruct((1, 2, own, k), jnp.float32),
        in_specs=[vmem, vmem, vmem, smem, smem],
        out_specs=vmem,
        scratch_shapes=[
            pltpu.VMEM((walkers, v, v), bf16),
            pltpu.VMEM((walkers, 1, v), jnp.int32),
            pltpu.VMEM((walkers, 1, v), jnp.int32),
            pltpu.SemaphoreType.DMA((3, walkers)),
            pltpu.SemaphoreType.DMA((3, walkers)),
            pltpu.VMEM((nf, v), jnp.int32),
            pltpu.VMEM((40, v), jnp.float32),
            pltpu.VMEM((40, v), jnp.float32),
            pltpu.VMEM((2 * v, 2 * v), bf16),
            pltpu.VMEM((k, 2 * v), bf16),
            pltpu.VMEM((k, 2 * v), bf16),
            pltpu.VMEM((2 * own, 2 * v), bf16),
            pltpu.VMEM((2 * own, 2 * v), bf16),
            pltpu.VMEM((2 * own, 2 * v), bf16),
            pltpu.VMEM((k, 2 * v), bf16),
        ],
        compiler_params=pltpu.CompilerParams(collective_id=0, has_side_effects=True),
    )(walker_m, vertex_times, vertex_labels, freq_index, q_index)


def solution(mesh):
    return jax.shard_map(
        local,
        mesh=mesh,
        in_specs=(
            P("walk", "blk", None, None),
            P("walk", "blk", None),
            P("walk", "blk", None),
            P(),
            P("blk"),
        ),
        out_specs=P("blk", None, "walk", None),
        check_vma=False,
    )
```

```python
import functools
import math

import jax
import jax.numpy as jnp
from jax import lax
from jax.experimental import pallas as pl
from jax.experimental.pallas import tpu as pltpu
from jax.sharding import PartitionSpec as P

SIDE = 6
TGRID = 1024
OFFSETS = (0, 1, -1, 2)
FORWARD = (2, 2, 3)


def sine(units):
    wrapped = ((units + 1024) & 2047) - 1024
    folded = jnp.where(wrapped > 512, 1024 - wrapped, wrapped)
    folded = jnp.where(wrapped < -512, -1024 - wrapped, folded)
    x = folded.astype(jnp.float32) * (math.pi / 1024.0)
    y = x * x
    total = jnp.full_like(y, 1.0 / math.factorial(13))
    for order in (11, 9, 7, 5, 3, 1):
        sign = -1.0 if (order // 2) % 2 else 1.0
        total = total * y + sign / math.factorial(order)
    return total * x


def sixth_turn(m):
    r = m - 6 * ((m * 10923) >> 16)
    half = jnp.where((r == 1) | (r == 5), 0.5, -0.5)
    cosine = jnp.where(r == 0, 1.0, jnp.where(r == 3, -1.0, half))
    root = math.sqrt(3.0) / 2.0
    side = jnp.where(r < 3, root, -root)
    return cosine.astype(jnp.float32), jnp.where((r == 0) | (r == 3), 0.0, side).astype(jnp.float32)


def visits(groups):
    around = sorted(range(1, groups), key=lambda z: min(z, groups - z))
    near = [(0, d) for d in range(len(OFFSETS))]
    far = [(z, 0) for z in around]
    return near + far + [(z, d) for z in around for d in range(1, len(OFFSETS))]


def kernel(
    groups, owners, m_in, t_in, l_in, freq_ref, q_ref, out_ref,
    m_ref, t_ref, l_ref, send_sem, recv_sem,
    odd, turn_c, turn_s, both, table, left_c, *buffers,
):
    order = visits(groups)
    walkers = len(order)
    w = lax.axis_index("walk")
    b = lax.axis_index("blk")

    def to_walk(z):
        return {"walk": lax.rem(w + groups - z, groups)}

    def to_blk(d):
        return {"blk": lax.rem(b + owners - OFFSETS[d], owners)}

    def copies(sources, slot, device):
        return [
            pltpu.make_async_remote_copy(
                src_ref=source,
                dst_ref=held.at[slot],
                send_sem=send_sem.at[kind, slot],
                recv_sem=recv_sem.at[kind, slot],
                device_id=device,
                device_id_type=pl.DeviceIdType.MESH,
            )
            for kind, (source, held) in enumerate(zip(sources, (m_ref, t_ref, l_ref)))
        ]

    own = (m_in.at[0, 0], t_in.at[0], l_in.at[0])

    def held_at(slot):
        return (m_ref.at[slot], t_ref.at[slot], l_ref.at[slot])

    def arrived(slot):
        for copy in copies(held_at(slot), slot, to_walk(1)):
            copy.wait_recv()

    barrier = pltpu.get_barrier_semaphore()
    peers = [{"walk": lax.rem(w + z, groups)} for z in range(1, groups)]
    reach = sorted({d % owners for d in OFFSETS + tuple(-d for d in OFFSETS)} - {0})
    peers += [{"blk": lax.rem(b + d, owners)} for d in reach]
    for peer in peers:
        pl.semaphore_signal(barrier, inc=1, device_id=peer, device_id_type=pl.DeviceIdType.MESH)
    def forward(z):
        slot = order.index((z, 0))
        arrived(slot)
        for d in range(1, len(OFFSETS)):
            for copy in copies(held_at(slot), order.index((z, d)), to_blk(d)):
                copy.start()

    m_ref[0] = m_in[0, 0]
    t_ref[0] = t_in[0]
    l_ref[0] = l_in[0]

    nf = freq_ref.shape[0]
    v = m_ref.shape[-1]
    nk = SIDE * SIDE
    own_k = out_ref.shape[2] // nf
    cols = out_ref.shape[3]
    first_k = w * own_k

    row = lax.broadcasted_iota(jnp.int32, (nf, v), 0)
    freq = jnp.zeros((nf, v), jnp.int32)
    for f in range(nf):
        freq = jnp.where(row == f, 2 * freq_ref[f] + 1, freq)
    odd[...] = freq
    both[...] = jnp.zeros_like(both)
    out_ref[...] = jnp.zeros_like(out_ref)
    q = q_ref[0]
    qx = (q * 43) >> 8
    qy = q - SIDE * qx

    def before(i):
        for turn, z in enumerate([z for z, d in order if z and not d]):
            @pl.when(i == FORWARD[min(turn, len(FORWARD) - 1)])
            def _(z=z):
                forward(z)

        first_far = order.index((0, len(OFFSETS) - 1)) + 1
        last_far = first_far + groups - 1

        @pl.when((i < first_far) | (i >= last_far))
        def _():
            arrived(i)

    def prepare(i, moved, left_a, left_b, right_b):
        matrix = m_ref[i]
        both[0:v, 0:v] = matrix
        both[v : 2 * v, v : 2 * v] = matrix
        times = t_ref[i]
        labels = l_ref[i]
        sx = (labels * 43) >> 8
        sy = labels - SIDE * sx
        k = lax.broadcasted_iota(jnp.int32, turn_c.shape, 0)
        kx = (k * 43) >> 8
        ky = k - SIDE * kx
        cosines, sines = sixth_turn(kx * sx + ky * sy)
        turn_c[...] = cosines
        turn_s[...] = sines
        cq, sq = sixth_turn(qx * sx + qy * sy)

        units = (odd[...] * times) & 2047
        ca = sine(units + 512)
        sa = sine(units)
        ca_q = ca * cq + sa * sq
        sa_q = sa * cq - ca * sq

        def turned(c, s, k):
            cb = turn_c[pl.ds(k, 1)]
            sb = turn_s[pl.ds(k, 1)]
            return c * cb + s * sb, s * cb - c * sb

        def put(ref, place, first, second, lanes):
            rows = slice(2 * nf * place, 2 * nf * (place + 1))
            ref[rows, lanes] = jnp.concatenate([first, second], axis=0).astype(jnp.bfloat16)

        low, high = slice(0, v), slice(v, 2 * v)
        for pair in range(nk // 2):
            c0, s0 = turned(ca, sa, 2 * pair)
            c1, s1 = turned(ca, sa, 2 * pair + 1)
            put(table, pair, c0, c1, low)
            put(table, pair, s0, s1, high)
            c0, s0 = turned(ca_q, sa_q, 2 * pair)
            c1, s1 = turned(ca_q, sa_q, 2 * pair + 1)
            put(moved, pair, c0, c1, low)
            put(moved, pair, s0, s1, high)
        for j in range(own_k):
            c, s = turned(ca, sa, first_k + j)
            put(left_b, j, c, -s, low)
            put(left_b, j, s, c, high)
            c, s = turned(ca_q, sa_q, first_k + j)
            put(left_c, j, c, s, low)
            put(left_c, j, s, -c, high)

        scale = 1.0 / (v * v * walkers)
        right_b[...] = jnp.dot(
            table[...], both[...], preferred_element_type=jnp.float32
        ).astype(jnp.bfloat16)
        product = jnp.dot(left_c[...], both[...], preferred_element_type=jnp.float32)
        left_a[...] = (product.astype(jnp.bfloat16).astype(jnp.float32) * scale).astype(jnp.bfloat16)

    def absorb(moved, left_a, left_b, right_b):
        contract = (((1,), (1,)), ((), ()))
        for start in range(0, cols, 256):
            stop = min(start + 256, cols)
            shifted = lax.dot_general(
                left_a[...], moved[start:stop], contract, preferred_element_type=jnp.float32
            )
            flipped = lax.dot_general(
                left_b[...], right_b[start:stop], contract, preferred_element_type=jnp.float32
            )
            for j in range(own_k):
                re = slice(2 * nf * j, 2 * nf * j + nf)
                im = slice(2 * nf * j + nf, 2 * nf * (j + 1))
                rows = slice(nf * j, nf * (j + 1))
                out_ref[0, 0, rows, start:stop] += (
                    shifted[re] * flipped[re] - shifted[im] * flipped[im]
                )
                out_ref[0, 1, rows, start:stop] += (
                    shifted[re] * flipped[im] + shifted[im] * flipped[re]
                )

    first, second = buffers[: len(buffers) // 2], buffers[len(buffers) // 2 :]
    prepare(0, *first)
    absorb(*first)
    pl.semaphore_wait(barrier, len(peers))
    for z, d in [o for o in order if o[0] and not o[1]] + [o for o in order if o[1] and not o[0]]:
        for copy in copies(own, order.index((z, d)), to_walk(z) if z else to_blk(d)):
            copy.start()

    before(1)
    prepare(1, *first)

    def step(turn, carry):
        i = 1 + 2 * turn
        for n, now, later in ((1, first, second), (2, second, first)):
            before(i + n)
            absorb(*now)
            prepare(i + n, *later)
        return carry

    lax.fori_loop(0, (walkers - 2) // 2, step, 0)
    absorb(*first)
    for slot in range(1, walkers):
        for copy in copies(held_at(slot), slot, to_walk(1)):
            copy.wait_send()


def local(walker_m, vertex_times, vertex_labels, freq_index, q_index):
    groups = lax.axis_size("walk")
    owners = lax.axis_size("blk")
    v = walker_m.shape[-1]
    nf = freq_index.shape[0]
    k = SIDE * SIDE * nf
    own = k // groups
    walkers = groups * len(OFFSETS)
    vmem = pl.BlockSpec(memory_space=pltpu.VMEM)
    smem = pl.BlockSpec(memory_space=pltpu.SMEM)
    bf16 = jnp.bfloat16
    return pl.pallas_call(
        functools.partial(kernel, groups, owners),
        out_shape=pltpu.VMEM((1, 2, own, k), jnp.float32),
        in_specs=[vmem, vmem, vmem, smem, smem],
        out_specs=vmem,
        scratch_shapes=[
            pltpu.VMEM((walkers, v, v), bf16),
            pltpu.VMEM((walkers, 1, v), jnp.int32),
            pltpu.VMEM((walkers, 1, v), jnp.int32),
            pltpu.SemaphoreType.DMA((3, walkers)),
            pltpu.SemaphoreType.DMA((3, walkers)),
            pltpu.VMEM((nf, v), jnp.int32),
            pltpu.VMEM((40, v), jnp.float32),
            pltpu.VMEM((40, v), jnp.float32),
            pltpu.VMEM((2 * v, 2 * v), bf16),
            pltpu.VMEM((k, 2 * v), bf16),
            pltpu.VMEM((2 * own, 2 * v), bf16),
        ]
        + 2
        * [
            pltpu.VMEM((k, 2 * v), bf16),
            pltpu.VMEM((2 * own, 2 * v), bf16),
            pltpu.VMEM((2 * own, 2 * v), bf16),
            pltpu.VMEM((k, 2 * v), bf16),
        ],
        compiler_params=pltpu.CompilerParams(collective_id=0, has_side_effects=True),
    )(walker_m, vertex_times, vertex_labels, freq_index, q_index)


def solution(mesh):
    return jax.shard_map(
        local,
        mesh=mesh,
        in_specs=(
            P("walk", "blk", None, None),
            P("walk", "blk", None),
            P("walk", "blk", None),
            P(),
            P("blk"),
        ),
        out_specs=P("blk", None, "walk", None),
        check_vma=False,
    )
```

```python
import functools
import math

import jax
import jax.numpy as jnp
from jax import lax
from jax.experimental import pallas as pl
from jax.experimental.pallas import tpu as pltpu
from jax.sharding import PartitionSpec as P

SIDE = 6
TGRID = 1024
OFFSETS = (0, 1, -1, 2)
FORWARD = (2, 3, 4)


def sine(units):
    wrapped = ((units + 1024) & 2047) - 1024
    folded = jnp.where(wrapped > 512, 1024 - wrapped, wrapped)
    folded = jnp.where(wrapped < -512, -1024 - wrapped, folded)
    x = folded.astype(jnp.float32) * (math.pi / 1024.0)
    y = x * x
    total = jnp.full_like(y, 1.0 / math.factorial(13))
    for order in (11, 9, 7, 5, 3, 1):
        sign = -1.0 if (order // 2) % 2 else 1.0
        total = total * y + sign / math.factorial(order)
    return total * x


def sixth_turn(m):
    r = m - 6 * ((m * 10923) >> 16)
    half = jnp.where((r == 1) | (r == 5), 0.5, -0.5)
    cosine = jnp.where(r == 0, 1.0, jnp.where(r == 3, -1.0, half))
    root = math.sqrt(3.0) / 2.0
    side = jnp.where(r < 3, root, -root)
    return cosine.astype(jnp.float32), jnp.where((r == 0) | (r == 3), 0.0, side).astype(jnp.float32)


def visits(groups):
    around = sorted(range(1, groups), key=lambda z: min(z, groups - z))
    near = [(0, d) for d in range(len(OFFSETS))]
    far = [(z, 0) for z in around]
    return near + far + [(z, d) for z in around for d in range(1, len(OFFSETS))]


def kernel(
    groups, owners, m_in, t_in, l_in, freq_ref, q_ref, out_ref,
    m_ref, t_ref, l_ref, send_sem, recv_sem,
    odd, turn_c, turn_s, both, table, moved, left_a, left_b, left_c, right_b,
):
    order = visits(groups)
    walkers = len(order)
    w = lax.axis_index("walk")
    b = lax.axis_index("blk")

    def to_walk(z):
        return {"walk": lax.rem(w + groups - z, groups)}

    def to_blk(d):
        return {"blk": lax.rem(b + owners - OFFSETS[d], owners)}

    def copies(sources, slot, device):
        return [
            pltpu.make_async_remote_copy(
                src_ref=source,
                dst_ref=held.at[slot],
                send_sem=send_sem.at[kind, slot],
                recv_sem=recv_sem.at[kind, slot],
                device_id=device,
                device_id_type=pl.DeviceIdType.MESH,
            )
            for kind, (source, held) in enumerate(zip(sources, (m_ref, t_ref, l_ref)))
        ]

    own = (m_in.at[0, 0], t_in.at[0], l_in.at[0])

    def held_at(slot):
        return (m_ref.at[slot], t_ref.at[slot], l_ref.at[slot])

    def arrived(slot):
        for copy in copies(held_at(slot), slot, to_walk(1)):
            copy.wait_recv()

    barrier = pltpu.get_barrier_semaphore()
    peers = [{"walk": lax.rem(w + z, groups)} for z in range(1, groups)]
    reach = sorted({d % owners for d in OFFSETS + tuple(-d for d in OFFSETS)} - {0})
    peers += [{"blk": lax.rem(b + d, owners)} for d in reach]
    for peer in peers:
        pl.semaphore_signal(barrier, inc=1, device_id=peer, device_id_type=pl.DeviceIdType.MESH)
    m_ref[0] = m_in[0, 0]
    t_ref[0] = t_in[0]
    l_ref[0] = l_in[0]
    both[...] = jnp.zeros_like(both)
    out_ref[...] = jnp.zeros_like(out_ref)
    pl.semaphore_wait(barrier, len(peers))
    for z, d in [o for o in order if o[0] and not o[1]] + [o for o in order if o[1] and not o[0]]:
        for copy in copies(own, order.index((z, d)), to_walk(z) if z else to_blk(d)):
            copy.start()

    def forward(z):
        slot = order.index((z, 0))
        arrived(slot)
        for d in range(1, len(OFFSETS)):
            for copy in copies(held_at(slot), order.index((z, d)), to_blk(d)):
                copy.start()


    nf = freq_ref.shape[0]
    v = m_ref.shape[-1]
    nk = SIDE * SIDE
    own_k = out_ref.shape[2] // nf
    cols = out_ref.shape[3]
    first_k = w * own_k

    row = lax.broadcasted_iota(jnp.int32, (nf, v), 0)
    freq = jnp.zeros((nf, v), jnp.int32)
    for f in range(nf):
        freq = jnp.where(row == f, 2 * freq_ref[f] + 1, freq)
    odd[...] = freq
    q = q_ref[0]
    qx = (q * 43) >> 8
    qy = q - SIDE * qx

    scale = 1.0 / (v * v * walkers)

    def step(visit, carry):
        swap = (lax.rem(b, 2) == 1) & ((visit == 1) | (visit == 2))
        i = jnp.where(swap, 3 - visit, visit)
        for turn, z in enumerate([z for z, d in order if z and not d]):
            @pl.when(visit == FORWARD[min(turn, len(FORWARD) - 1)])
            def _(z=z):
                forward(z)

        first_far = order.index((0, len(OFFSETS) - 1)) + 1
        last_far = first_far + groups - 1

        @pl.when(((visit > 0) & (visit < first_far)) | (visit >= last_far))
        def _():
            arrived(i)

        matrix = m_ref[i]
        both[0:v, 0:v] = matrix
        both[v : 2 * v, v : 2 * v] = matrix
        times = t_ref[i]
        labels = l_ref[i]
        sx = (labels * 43) >> 8
        sy = labels - SIDE * sx
        k = lax.broadcasted_iota(jnp.int32, turn_c.shape, 0)
        kx = (k * 43) >> 8
        ky = k - SIDE * kx
        cosines, sines = sixth_turn(kx * sx + ky * sy)
        turn_c[...] = cosines
        turn_s[...] = sines
        cq, sq = sixth_turn(qx * sx + qy * sy)

        units = (odd[...] * times) & 2047
        ca = sine(units + 512)
        sa = sine(units)
        ca_q = ca * cq + sa * sq
        sa_q = sa * cq - ca * sq

        def turned(c, s, k):
            cb = turn_c[pl.ds(k, 1)]
            sb = turn_s[pl.ds(k, 1)]
            return c * cb + s * sb, s * cb - c * sb

        def put(ref, place, first, second, lanes):
            rows = slice(2 * nf * place, 2 * nf * (place + 1))
            ref[rows, lanes] = jnp.concatenate([first, second], axis=0).astype(jnp.bfloat16)

        low, high = slice(0, v), slice(v, 2 * v)
        for pair in range(nk // 2):
            c0, s0 = turned(ca, sa, 2 * pair)
            c1, s1 = turned(ca, sa, 2 * pair + 1)
            put(table, pair, c0, c1, low)
            put(table, pair, s0, s1, high)
            c0, s0 = turned(ca_q, sa_q, 2 * pair)
            c1, s1 = turned(ca_q, sa_q, 2 * pair + 1)
            put(moved, pair, c0, c1, low)
            put(moved, pair, s0, s1, high)
        for j in range(own_k):
            c, s = turned(ca, sa, first_k + j)
            put(left_b, j, c, -s, low)
            put(left_b, j, s, c, high)
            c, s = turned(ca_q, sa_q, first_k + j)
            put(left_c, j, c, s, low)
            put(left_c, j, s, -c, high)

        right_b[...] = jnp.dot(
            table[...], both[...], preferred_element_type=jnp.float32
        ).astype(jnp.bfloat16)
        product = jnp.dot(left_c[...], both[...], preferred_element_type=jnp.float32)
        left_a[...] = (product.astype(jnp.bfloat16).astype(jnp.float32) * scale).astype(jnp.bfloat16)

        contract = (((1,), (1,)), ((), ()))
        for start in range(0, cols, 256):
            stop = min(start + 256, cols)
            shifted = lax.dot_general(
                left_a[...], moved[start:stop], contract, preferred_element_type=jnp.float32
            )
            flipped = lax.dot_general(
                left_b[...], right_b[start:stop], contract, preferred_element_type=jnp.float32
            )
            for j in range(own_k):
                re = slice(2 * nf * j, 2 * nf * j + nf)
                im = slice(2 * nf * j + nf, 2 * nf * (j + 1))
                rows = slice(nf * j, nf * (j + 1))
                out_ref[0, 0, rows, start:stop] += (
                    shifted[re] * flipped[re] - shifted[im] * flipped[im]
                )
                out_ref[0, 1, rows, start:stop] += (
                    shifted[re] * flipped[im] + shifted[im] * flipped[re]
                )
        return carry

    lax.fori_loop(0, walkers, step, 0)
    for slot in range(1, walkers):
        for copy in copies(held_at(slot), slot, to_walk(1)):
            copy.wait_send()


def local(walker_m, vertex_times, vertex_labels, freq_index, q_index):
    groups = lax.axis_size("walk")
    owners = lax.axis_size("blk")
    v = walker_m.shape[-1]
    nf = freq_index.shape[0]
    k = SIDE * SIDE * nf
    own = k // groups
    walkers = groups * len(OFFSETS)
    vmem = pl.BlockSpec(memory_space=pltpu.VMEM)
    smem = pl.BlockSpec(memory_space=pltpu.SMEM)
    bf16 = jnp.bfloat16
    return pl.pallas_call(
        functools.partial(kernel, groups, owners),
        out_shape=pltpu.VMEM((1, 2, own, k), jnp.float32),
        in_specs=[vmem, vmem, vmem, smem, smem],
        out_specs=vmem,
        scratch_shapes=[
            pltpu.VMEM((walkers, v, v), bf16),
            pltpu.VMEM((walkers, 1, v), jnp.int32),
            pltpu.VMEM((walkers, 1, v), jnp.int32),
            pltpu.SemaphoreType.DMA((3, walkers)),
            pltpu.SemaphoreType.DMA((3, walkers)),
            pltpu.VMEM((nf, v), jnp.int32),
            pltpu.VMEM((40, v), jnp.float32),
            pltpu.VMEM((40, v), jnp.float32),
            pltpu.VMEM((2 * v, 2 * v), bf16),
            pltpu.VMEM((k, 2 * v), bf16),
            pltpu.VMEM((k, 2 * v), bf16),
            pltpu.VMEM((2 * own, 2 * v), bf16),
            pltpu.VMEM((2 * own, 2 * v), bf16),
            pltpu.VMEM((2 * own, 2 * v), bf16),
            pltpu.VMEM((k, 2 * v), bf16),
        ],
        compiler_params=pltpu.CompilerParams(collective_id=0, has_side_effects=True),
    )(walker_m, vertex_times, vertex_labels, freq_index, q_index)


def solution(mesh):
    return jax.shard_map(
        local,
        mesh=mesh,
        in_specs=(
            P("walk", "blk", None, None),
            P("walk", "blk", None),
            P("walk", "blk", None),
            P(),
            P("blk"),
        ),
        out_specs=P("blk", None, "walk", None),
        check_vma=False,
    )
```
